256 devices in a mesh: dp: 8 (over z_hi, x), ha: 4 (over y), wa: 8 (over z_lo, core).
Axes of the slice: x: 4, y: 4, z: 8 (z_hi: 2, z_lo: 4; z = z_hi * 4 + z_lo), core: 2. Of those that a mesh axis runs over, the one named last changes fastest.
Arguments:
- queries: bfloat16 [8, 1, 4, 8, 144, 768], P('dp', None, 'ha', 'wa'), may hold values from -5 to 5
- key_tiles: bfloat16 [8, 1, 4, 8, 144, 768], P('dp', None, 'ha', 'wa'), may hold values from -5 to 5
- value_tiles: bfloat16 [8, 1, 4, 8, 144, 768], P('dp', None, 'ha', 'wa'), may hold values from -6 to 6
- out_grad: bfloat16 [8, 1, 4, 8, 144, 1536], P('dp', None, 'ha', 'wa'), may hold values from -8 to 8
- w_out: bfloat16 [1536, 768], replicated, may hold values from -0.21875 to 0.21875
- reaches: int32 [6, 6], replicated, may hold values from 0 to 1, as said below
Outputs:
- grad_query: bfloat16 [8, 1, 4, 8, 144, 768], P('dp', None, 'ha', 'wa')
- grad_key: bfloat16 [8, 1, 4, 8, 144, 768], P('dp', None, 'ha', 'wa')
- grad_value: bfloat16 [8, 1, 4, 8, 144, 768], P('dp', None, 'ha', 'wa')
- grad_w_out: float32 [1536, 768], P(('dp', 'ha', 'wa'))
The draws below stay inside these ranges and needn't reach their ends.
Inputs may be any that keep to these rules, and one draw needn't show every extreme that they name: `reaches`: some head has every entry 1, and some other head has every entry 0.
All inputs are finite; a program needn't handle non-finite values.
Results may differ from the reference program's by a relative error of at most 0.018.
Values may be sent and summed in bfloat16 or wider, within the bound.
No kernel may reach another device: no remote copies, remote signals or barrier semaphores. Data moves between devices by JAX's collectives and lax.ppermute only.
A program may use at most 128 MiB of HBM per device.

```python
import math
import jax
import jax.numpy as jnp
from jax import lax

D = 1536
HEADS = 6
HD = 128
NT = 1
TILE = 144
HQ = 768
B = 8
NH = 4
NW = 8


def draw_queries(key, part):
    shape_rows = (B * NT * NH * NW * TILE, HQ)
    own_key = jax.random.fold_in(key, 11)
    flat_rows = jax.random.truncated_normal(own_key, -4.0, 4.0, shape_rows, jnp.float32)
    return flat_rows.reshape(B, NT, NH, NW, TILE, HQ).astype(jnp.bfloat16)


def draw_key_tiles(key, part):
    shape_rows = (B * NT * NH * NW * TILE, HQ)
    own_key = jax.random.fold_in(key, 12)
    flat_rows = jax.random.truncated_normal(own_key, -4.0, 4.0, shape_rows, jnp.float32)
    return flat_rows.reshape(B, NT, NH, NW, TILE, HQ).astype(jnp.bfloat16)


def draw_reaches(key, part):
    first_head = jax.random.randint(jax.random.fold_in(key, 21), (), 0, HEADS)
    second_head = (first_head + 1 + jax.random.randint(jax.random.fold_in(key, 22), (), 0, HEADS - 1)) % HEADS
    random_bits = jax.random.randint(jax.random.fold_in(key, 23), (HEADS, 6), 0, 2)
    head_ids = jnp.arange(HEADS)[:, None]
    chosen = jnp.where(head_ids == first_head, 1, jnp.where(head_ids == second_head, 0, random_bits))
    return chosen.astype(jnp.int32)


def spiked(result, key, source, target, blocks, factor):
    def block_of(position):
        return (jnp.arange(result.shape[position]) // (result.shape[position] // blocks)).reshape((-1,) + (1,) * (result.ndim - 1 - position))

    one_side = jax.random.permutation(key, blocks)[block_of(target)]
    other_side = (block_of(target) + blocks // 2) % blocks
    return jnp.where((block_of(source) == one_side) | (block_of(source) == other_side), factor * result, result)


def steps_of(stream_key, shape, shards, least, top_value):
    loudness = 1.0
    for axis_at, shards_of in shards:
        heights = jax.random.uniform(jax.random.fold_in(jax.random.fold_in(stream_key, 6), axis_at), (shards_of,), jnp.float32, least / len(shards), top_value / len(shards))
        loudness = loudness * jnp.repeat(jnp.exp(heights), shape[axis_at] // shards_of).reshape((-1,) + (1,) * (len(shape) - 1 - axis_at))
    return loudness


def gaussian(key, extent, deviation, limit, shards=(), kind=jnp.bfloat16):
    result = jax.random.normal(key, extent, jnp.float32) * deviation
    if len(shards) > 0:
        result = steps_of(key, extent, shards, -0.22, 0.18) * result
    return jnp.clip(result, min=-limit, max=limit).astype(kind)


def gaussian_with(rng, extent, spread, most, cuts, heavy, dtype=jnp.bfloat16):
    result = spread * jax.random.normal(rng, extent, jnp.float32)
    if cuts:
        result = result * steps_of(rng, extent, cuts, -0.22, 0.18)
    return jnp.clip(spiked(result, jax.random.fold_in(rng, 3), *heavy), -most, most).astype(dtype)


def setup_inputs(seed: int = 0) -> dict:
    arg_keys = jax.random.split(jax.random.key(seed), 7)
    return {
        "queries": draw_queries(jax.random.fold_in(arg_keys[6], 71), 0),
        "key_tiles": draw_key_tiles(jax.random.fold_in(arg_keys[6], 71), 0),
        "value_tiles": gaussian(arg_keys[2], (B, NT, NH, NW, TILE, HQ), 1.0, 6.0, ((0, 8), (2, 4), (3, 8))),
        "out_grad": gaussian_with(arg_keys[3], (B, NT, NH, NW, TILE, D), 1.0, 8.0, ((0, 8), (2, 4), (3, 8)), (3, 5, 8, 2.0)),
        "w_out": gaussian(arg_keys[4], (D, HQ), HQ ** -0.5, 0.21875),
        "reaches": draw_reaches(jax.random.fold_in(arg_keys[6], 71), 0),
    }


def neighbours(tile_field):
    padded = jnp.pad(tile_field, ((0, 0), (1, 1), (1, 1), (0, 0), (0, 0)))
    stacked = jnp.stack([jnp.stack([padded[:, row_off:row_off + NH, col_off:col_off + NW] for col_off in range(3)], 0) for row_off in range(3)], 0)
    arranged = jnp.transpose(stacked, (3, 4, 2, 0, 1, 5, 6))
    return arranged.reshape(NH, NW, NT * 9 * TILE, tile_field.shape[-1])

def fold_back(contrib):
    channels = contrib.shape[-1]
    pieces = contrib.reshape(NH, NW, NT, 3, 3, TILE, channels)
    summed = jnp.zeros((NT, NH + 2, NW + 2, TILE, channels), jnp.float32)
    for row_off in range(3):
        for col_off in range(3):
            summed = summed.at[:, row_off:row_off + NH, col_off:col_off + NW].add(jnp.transpose(pieces[:, :, :, row_off, col_off], (2, 0, 1, 3, 4)))
    return summed[:, 1:NH + 1, 1:NW + 1]

def allowed_pairs(reach_row):
    time_ids = jnp.arange(NT)
    t_delta = time_ids[None, :] - time_ids[:, None]
    time_ok = (t_delta >= -reach_row[0]) & (t_delta <= reach_row[1])
    offsets = jnp.arange(3) - 1
    row_pos = jnp.arange(NH)[:, None] + offsets[None, :]
    row_ok = ((offsets >= -reach_row[2]) & (offsets <= reach_row[3]))[None, :] & (row_pos >= 0) & (row_pos < NH)
    col_pos = jnp.arange(NW)[:, None] + offsets[None, :]
    col_ok = ((offsets >= -reach_row[4]) & (offsets <= reach_row[5]))[None, :] & (col_pos >= 0) & (col_pos < NW)
    tile_pairs = time_ok[None, None, :, :, None, None] & row_ok[:, None, None, None, :, None] & col_ok[None, :, None, None, None, :]
    expanded = jnp.broadcast_to(tile_pairs[:, :, :, None, :, :, :, None], (NH, NW, NT, TILE, NT, 3, 3, TILE))
    return expanded.reshape(NH, NW, NT * TILE, NT * 9 * TILE)

def to_columns(tile_field):
    return jnp.transpose(tile_field, (1, 2, 0, 3, 4)).reshape(NH, NW, NT * TILE, tile_field.shape[-1])

def from_columns(column_field):
    return jnp.transpose(column_field.reshape(NH, NW, NT, TILE, column_field.shape[-1]), (2, 0, 1, 3, 4))

def sample_grads(inputs, w_out, reaches):
    query_part, key_part, value_part, grad_part = inputs
    softmax_scale = 1.0 / math.sqrt(HD)
    grad_rows = grad_part.astype(jnp.float32).reshape(-1, D)
    grad_attn = jnp.dot(grad_rows, w_out.astype(jnp.float32)).astype(jnp.bfloat16).reshape(NT, NH, NW, TILE, HQ)
    attn_list, gq_list, gk_list, gv_list = ([], [], [], [])
    for head_index in range(HEADS):
        col_start = head_index * HD
        col_stop = col_start + HD
        query_head = to_columns(query_part[..., col_start:col_stop].astype(jnp.float32))
        grad_head = to_columns(grad_attn[..., col_start:col_stop].astype(jnp.float32))
        key_near = neighbours(key_part[..., col_start:col_stop].astype(jnp.float32))
        value_near = neighbours(value_part[..., col_start:col_stop].astype(jnp.float32))
        allowed = allowed_pairs(reaches[head_index])
        scores = jnp.einsum('ijad,ijbd->ijab', query_head, key_near) * softmax_scale
        masked = jnp.where(allowed, scores, -jnp.inf)
        row_peak = lax.optimization_barrier(jnp.max(masked, axis=-1, keepdims=True))
        exp_terms = jnp.exp(masked - row_peak)
        prob_rows = exp_terms / lax.optimization_barrier(jnp.sum(exp_terms, axis=-1, keepdims=True))
        probs_wide = lax.optimization_barrier(prob_rows.astype(jnp.bfloat16)).astype(jnp.float32)
        attn_head = jnp.einsum('ijab,ijbd->ijad', probs_wide, value_near).astype(jnp.bfloat16)
        row_delta = lax.optimization_barrier(jnp.sum(grad_head * attn_head.astype(jnp.float32), axis=-1, keepdims=True))
        grad_probs = jnp.einsum('ijad,ijbd->ijab', grad_head, value_near)
        grad_scores = lax.optimization_barrier((prob_rows * (grad_probs - row_delta)).astype(jnp.bfloat16)).astype(jnp.float32)
        grad_q_head = (jnp.einsum('ijab,ijbd->ijad', grad_scores, key_near) * softmax_scale).astype(jnp.bfloat16)
        grad_k_near = jnp.einsum('ijab,ijad->ijbd', grad_scores, query_head) * softmax_scale
        grad_v_near = jnp.einsum('ijab,ijad->ijbd', probs_wide, grad_head)
        attn_list.append(from_columns(attn_head))
        gq_list.append(from_columns(grad_q_head))
        gk_list.append(fold_back(grad_k_near))
        gv_list.append(fold_back(grad_v_near))
    attended = jnp.concatenate(attn_list, axis=-1)
    grad_q = jnp.concatenate(gq_list, axis=-1)
    grad_k = jnp.concatenate(gk_list, axis=-1).astype(jnp.bfloat16)
    grad_v = jnp.concatenate(gv_list, axis=-1).astype(jnp.bfloat16)
    grad_w = jnp.dot(grad_rows.T, attended.astype(jnp.float32).reshape(-1, HQ))
    return (grad_q, grad_k, grad_v, grad_w)

def reference(queries, key_tiles, value_tiles, out_grad, w_out, reaches):

    def per_sample(inputs):
        return sample_grads(inputs, w_out, reaches)
    grad_q, grad_k, grad_v, grad_w = lax.map(per_sample, (queries, key_tiles, value_tiles, out_grad))
    return (grad_q, grad_k, grad_v, lax.optimization_barrier(jnp.sum(grad_w, axis=0)))
```

```python
import math

import jax
import jax.numpy as jnp
from jax import lax
from jax.experimental import pallas as pl
from jax.experimental.pallas import tpu as pltpu
from jax.sharding import PartitionSpec as P

HEADS = 6
HD = 128
TILE = 144
SENT = HEADS - 1
ROWS = 3 * TILE
F32 = jnp.float32
BF16 = jnp.bfloat16
SCALE = 1.0 / math.sqrt(HD)
SCALE2 = SCALE * math.log2(math.e)
LOW = -1e30

SMEM = pl.BlockSpec(memory_space=pltpu.SMEM)
VMEM = pl.BlockSpec(memory_space=pltpu.VMEM)


def nt_dot(a, b):
    return lax.dot_general(a, b, (((1,), (1,)), ((), ())), preferred_element_type=F32)


def tn_dot(a, b):
    return lax.dot_general(a, b, (((0,), (0,)), ((), ())), preferred_element_type=F32)


def nn_dot(a, b):
    return jnp.dot(a, b, preferred_element_type=F32)


def lone_head(reaches):
    lone = jnp.int32(HEADS)
    for head in reversed(range(HEADS)):
        total = reaches[head, 0]
        for side in range(1, 6):
            total = total + reaches[head, side]
        lone = jnp.where(total == 0, jnp.int32(head), lone)
    return lone


def columns(head):
    return pl.ds(pl.multiple_of(head * HD, HD), HD)


def head_of(slot, lone):
    return slot + (slot >= lone).astype(jnp.int32)


def biases(reaches, place, head):
    row, col = place[0], place[1]
    row_count, col_count = place[2], place[3]
    up = jnp.where((reaches[head, 2] > 0) & (row > 0), 0.0, LOW)
    down = jnp.where((reaches[head, 3] > 0) & (row < row_count - 1), 0.0, LOW)
    left = jnp.where((reaches[head, 4] > 0) & (col > 0), 0.0, LOW)
    right = jnp.where((reaches[head, 5] > 0) & (col < col_count - 1), 0.0, LOW)
    lane = lax.broadcasted_iota(jnp.int32, (1, ROWS), 1)
    by_row = jnp.where(lane < TILE, up, jnp.where(lane < 2 * TILE, 0.0, down))
    return (jnp.minimum(by_row, left), by_row, jnp.minimum(by_row, right))


def pack_kernel(reaches, keys, values, packed):
    lone = lone_head(reaches)
    for slot in range(SENT):
        cols = columns(head_of(jnp.int32(slot), lone))
        packed[slot, :, :HD] = keys[:, cols]
        packed[slot, :, HD:] = values[:, cols]


def forward_kernel(reaches, place, queries, keys, values, left, mid, right, attended, norms):
    lone = lone_head(reaches)

    def one(slot, carry):
        head = head_of(slot, lone)
        cols = columns(head)
        query = queries[:, cols]
        scores = [
            nt_dot(query, block[slot, :, :HD]) + bias
            for block, bias in zip((left, mid, right), biases(reaches, place, head))
        ]
        peak = jnp.max(jnp.maximum(jnp.maximum(scores[0], scores[1]), scores[2]), axis=1, keepdims=True)
        terms = [jnp.exp2((s - peak) * SCALE2) for s in scores]
        total = jnp.sum(terms[0] + terms[1] + terms[2], axis=1, keepdims=True)
        sums = sum(
            nn_dot(t.astype(BF16), block[slot, :, HD:]) for t, block in zip(terms, (left, mid, right))
        )
        attended[:, cols] = (sums / total).astype(BF16)
        norms[slot] = jnp.broadcast_to(peak * SCALE2 + jnp.log2(total), (TILE, HD))
        return carry

    lax.fori_loop(0, SENT, one, 0)
    cols = columns(lone)
    scores = nt_dot(queries[:, cols], keys[:, cols])
    peak = jnp.max(scores, axis=1, keepdims=True)
    terms = jnp.exp2((scores - peak) * SCALE2)
    total = jnp.sum(terms, axis=1, keepdims=True)
    attended[:, cols] = (nn_dot(terms.astype(BF16), values[:, cols]) / total).astype(BF16)
    norms[SENT] = jnp.broadcast_to(peak * SCALE2 + jnp.log2(total), (TILE, HD))


def backward_kernel(
    reaches, place, queries, keys, values, grads, attended, norms, left, mid, right,
    grad_query, g_left, g_mid, g_right, g_lone,
):
    lone = lone_head(reaches)

    def one(slot, carry):
        head = head_of(slot, lone)
        cols = columns(head)
        query = queries[:, cols]
        grad = grads[:, cols]
        norm = norms[slot][:, :1]
        delta = jnp.sum(grad.astype(F32) * attended[:, cols].astype(F32), axis=1, keepdims=True)
        total = jnp.zeros((TILE, HD), F32)
        for block, bias, out in zip(
            (left, mid, right), biases(reaches, place, head), (g_left, g_mid, g_right)
        ):
            key = block[slot, :, :HD]
            value = block[slot, :, HD:]
            probs = jnp.exp2((nt_dot(query, key) + bias) * SCALE2 - norm)
            slopes = (probs * (nt_dot(grad, value) - delta)).astype(BF16)
            total = total + nn_dot(slopes, key)
            out[slot, :, :HD] = (tn_dot(slopes, query) * SCALE).astype(BF16)
            out[slot, :, HD:] = tn_dot(probs.astype(BF16), grad).astype(BF16)
        grad_query[:, cols] = (total * SCALE).astype(BF16)
        return carry

    lax.fori_loop(0, SENT, one, 0)
    cols = columns(lone)
    query = queries[:, cols]
    grad = grads[:, cols]
    key = keys[:, cols]
    delta = jnp.sum(grad.astype(F32) * attended[:, cols].astype(F32), axis=1, keepdims=True)
    probs = jnp.exp2(nt_dot(query, key) * SCALE2 - norms[SENT][:, :1])
    slopes = (probs * (nt_dot(grad, values[:, cols]) - delta)).astype(BF16)
    grad_query[:, cols] = (nn_dot(slopes, key) * SCALE).astype(BF16)
    g_lone[:, :HD] = (tn_dot(slopes, query) * SCALE).astype(BF16)
    g_lone[:, HD:] = tn_dot(probs.astype(BF16), grad).astype(BF16)


def width_sum_kernel(g_mid, from_right, from_left, own, to_up, to_down):
    for slot in range(SENT):
        total = (
            g_mid[slot].astype(F32) + from_right[slot].astype(F32) + from_left[slot].astype(F32)
        )
        to_up[slot] = total[:TILE].astype(BF16)
        own[slot] = total[TILE : 2 * TILE]
        to_down[slot] = total[2 * TILE :].astype(BF16)


def height_sum_kernel(reaches, own, from_down, from_up, g_lone, grad_key, grad_value):
    lone = lone_head(reaches)
    for slot in range(SENT):
        cols = columns(head_of(jnp.int32(slot), lone))
        total = own[slot] + from_down[slot].astype(F32) + from_up[slot].astype(F32)
        grad_key[:, cols] = total[:, :HD].astype(BF16)
        grad_value[:, cols] = total[:, HD:].astype(BF16)
    cols = columns(lone)
    grad_key[:, cols] = g_lone[:, :HD]
    grad_value[:, cols] = g_lone[:, HD:]


def call(kernel, outs, specs, flops=0):
    return pl.pallas_call(
        kernel,
        out_shape=[jax.ShapeDtypeStruct(shape, dtype) for shape, dtype in outs],
        in_specs=specs,
        out_specs=[VMEM] * len(outs),
        cost_estimate=pl.CostEstimate(flops=flops, transcendentals=0, bytes_accessed=1 << 20),
    )


def shifted(block, axis, distance):
    devices = range(lax.axis_size(axis))
    route = [(i - distance, i) for i in devices if i - distance in devices]
    return lax.ppermute(block, axis, route)


def row_order(model_width, dp, ha, wa):
    import numpy as np

    width = model_width // (dp * ha * wa)
    index = np.arange(model_width).reshape(2, dp // 2, ha, wa // 2, 2, width)
    return index.transpose(4, 1, 2, 0, 3, 5).reshape(-1)


def exchanged(array, axes, groups, size):
    parts = array.reshape(size, array.shape[0] // size, array.shape[1])
    parts = lax.all_to_all(parts, axes, 0, 0, axis_index_groups=groups, tiled=True)
    return jnp.sum(parts.astype(F32), axis=0)


def shards(queries, key_tiles, value_tiles, out_grad, w_out, reaches):
    shape = queries.shape
    width = shape[5]
    model_width = out_grad.shape[5]
    dp, ha, wa = (lax.axis_size(axis) for axis in ("dp", "ha", "wa"))
    place = jnp.stack(
        [lax.axis_index("ha"), lax.axis_index("wa"), jnp.int32(ha), jnp.int32(wa)]
    ).astype(jnp.int32)
    queries = queries.reshape(TILE, width)
    keys = key_tiles.reshape(TILE, width)
    values = value_tiles.reshape(TILE, width)
    grad_rows = out_grad.reshape(TILE, model_width)

    tile = (SENT, TILE, 2 * HD)
    rows = (SENT, ROWS, 2 * HD)
    (packed,) = call(pack_kernel, [(tile, BF16)], [SMEM, VMEM, VMEM])(reaches, keys, values)
    up = shifted(packed, "ha", 1)
    down = shifted(packed, "ha", -1)
    mid = jnp.concatenate([up, packed, down], axis=1)
    left = shifted(mid, "wa", 1)
    right = shifted(mid, "wa", -1)

    grads = jnp.dot(grad_rows, w_out, preferred_element_type=F32).astype(BF16)
    order = row_order(model_width, dp, ha, wa)
    select = (jnp.arange(model_width)[:, None] == order[None, :]).astype(BF16)
    sorted_rows = jnp.dot(grad_rows, select, preferred_element_type=F32).astype(BF16)
    halves = sorted_rows.reshape(TILE, 2, model_width // 2)
    core = lax.axis_index("wa") % 2
    pair = [(i, i ^ 1) for i in range(wa)]
    mine = jnp.where(core == 0, halves[:, 0], halves[:, 1])
    other = jnp.where(core == 0, halves[:, 1], halves[:, 0])
    partner_rows = lax.ppermute(other, "wa", pair)
    both_rows = jnp.concatenate([mine, partner_rows], axis=0)

    attended, norms = call(
        forward_kernel,
        [((TILE, width), BF16), ((HEADS, TILE, HD), F32)],
        [SMEM, SMEM] + [VMEM] * 6,
        flops=10**9,
    )(reaches, place, queries, keys, values, left, mid, right)

    both_attended = jnp.concatenate([attended, lax.ppermute(attended, "wa", pair)], axis=0)
    product = lax.dot_general(
        both_rows, both_attended, (((0,), (0,)), ((), ())), preferred_element_type=F32
    ).astype(BF16)
    half = dp // 2
    x_groups = [[z * half + x for x in range(half)] for z in range(2)]
    summed = exchanged(product, "dp", x_groups, half).astype(BF16)
    summed = exchanged(summed, "ha", None, ha).astype(BF16)
    z_groups = [
        [(z * half + x) * wa + w * 2 + c for z in range(2) for w in range(wa // 2)]
        for x in range(half)
        for c in range(2)
    ]
    grad_w_out = exchanged(summed, ("dp", "wa"), z_groups, wa)

    grad_query, g_left, g_mid, g_right, g_lone = call(
        backward_kernel,
        [((TILE, width), BF16), (rows, BF16), (rows, BF16), (rows, BF16), ((TILE, 2 * HD), BF16)],
        [SMEM, SMEM] + [VMEM] * 9,
        flops=2 * 10**9,
    )(reaches, place, queries, keys, values, grads, attended, norms, left, mid, right)
    from_right = shifted(g_left, "wa", -1)
    from_left = shifted(g_right, "wa", 1)
    own, to_up, to_down = call(
        width_sum_kernel, [(tile, F32), (tile, BF16), (tile, BF16)], [VMEM] * 3
    )(g_mid, from_right, from_left)
    from_down = shifted(to_up, "ha", -1)
    from_up = shifted(to_down, "ha", 1)
    grad_key, grad_value = call(
        height_sum_kernel, [((TILE, width), BF16)] * 2, [SMEM] + [VMEM] * 4
    )(reaches, own, from_down, from_up, g_lone)
    return (
        grad_query.reshape(shape), grad_key.reshape(shape), grad_value.reshape(shape), grad_w_out,
    )


def solution(mesh):
    tiles = P("dp", None, "ha", "wa", None, None)
    return jax.shard_map(
        shards,
        mesh=mesh,
        in_specs=(tiles, tiles, tiles, tiles, P(), P()),
        out_specs=(tiles, tiles, tiles, P(("dp", "ha", "wa"), None)),
        check_vma=False,
    )
```

```python
import functools
import math

import jax
import jax.numpy as jnp
from jax import lax
from jax.experimental import pallas as pl
from jax.experimental.pallas import tpu as pltpu
from jax.sharding import Mesh
from jax.sharding import PartitionSpec as P

HEADS = 6
HD = 128
TILE = 144
SENT = HEADS - 1
F32 = jnp.float32
BF16 = jnp.bfloat16
SCALE = 1.0 / math.sqrt(HD)
SCALE2 = SCALE * math.log2(math.e)
LOW = -1e30
WIDTH = ("zl", "core")

SMEM = pl.BlockSpec(memory_space=pltpu.SMEM)
VMEM = pl.BlockSpec(memory_space=pltpu.VMEM)
HBM = pl.BlockSpec(memory_space=pltpu.HBM)


def nt_dot(a, b):
    return lax.dot_general(a, b, (((1,), (1,)), ((), ())), preferred_element_type=F32)


def tn_dot(a, b):
    return lax.dot_general(a, b, (((0,), (0,)), ((), ())), preferred_element_type=F32)


def nn_dot(a, b):
    return jnp.dot(a, b, preferred_element_type=F32)


def lone_head(reaches):
    lone = jnp.int32(HEADS)
    for head in reversed(range(HEADS)):
        total = reaches[head, 0]
        for side in range(1, 6):
            total = total + reaches[head, side]
        lone = jnp.where(total == 0, jnp.int32(head), lone)
    return lone


def columns(head):
    return pl.ds(pl.multiple_of(head * HD, HD), HD)


def head_of(slot, lone):
    return slot + (slot >= lone).astype(jnp.int32)


def sides(reaches, head, column, index, count):
    before = jnp.where((reaches[head, column] > 0) & (index > 0), 0.0, LOW)
    after = jnp.where((reaches[head, column + 1] > 0) & (index < count - 1), 0.0, LOW)
    even = index % 2 == 0
    return jnp.where(even, after, before), jnp.where(even, before, after)


def width_bias(reaches, place, head):
    near, far = sides(reaches, head, 4, place[1], place[3])
    lane = lax.broadcasted_iota(jnp.int32, (1, 3 * TILE), 1)
    return jnp.where(lane < TILE, near, jnp.where(lane < 2 * TILE, 0.0, far))


def rows_bias(reaches, place, head):
    near, far = sides(reaches, head, 4, place[1], place[3])
    row_near, row_far = sides(reaches, head, 2, place[0], place[2])
    lane = lax.broadcasted_iota(jnp.int32, (1, 6 * TILE), 1)
    column = jnp.where(lane < 2 * TILE, near, jnp.where(lane < 4 * TILE, 0.0, far))
    start = jnp.where(lane < 2 * TILE, 0, jnp.where(lane < 4 * TILE, 2 * TILE, 4 * TILE))
    return jnp.minimum(column, jnp.where(lane - start < TILE, row_near, row_far))


def keys_of(tiles, slot):
    return jnp.concatenate([tile[slot, :, :HD] for tile in tiles], axis=0)


def values_of(tiles, slot):
    return jnp.concatenate([tile[slot, :, HD:] for tile in tiles], axis=0)


def pack_kernel(reaches, keys, values, packed, arrived):
    lone = lone_head(reaches)
    copies = []
    for slot in range(SENT):
        cols = columns(head_of(jnp.int32(slot), lone))
        for index, source in enumerate((keys, values)):
            copies.append(
                pltpu.make_async_copy(
                    source.at[:, cols],
                    packed.at[slot, :, index * HD : (index + 1) * HD],
                    arrived.at[slot, index],
                )
            )
    for copy in copies:
        copy.start()
    for copy in copies:
        copy.wait()


def stack_kernel(near, far, both):
    both[:, :TILE] = near[...]
    both[:, TILE:] = far[...]


def rows_kernel(step, place, out_grad, w_out, grads, mine, other, rows, weights, arrived):
    rows_copy = pltpu.make_async_copy(out_grad, rows, arrived.at[0])
    weights_copy = pltpu.make_async_copy(w_out, weights, arrived.at[1])
    rows_copy.start()
    weights_copy.start()
    size, half = rows.shape[1] // 4, rows.shape[1] // 2
    column = lax.broadcasted_iota(jnp.int32, (size, half), 1)
    row = lax.broadcasted_iota(jnp.int32, (size, 1), 0)
    wanted = row + step * ((row * ((1 << 18) // step + 1)) >> 18)
    core = place[1] % 2
    rows_copy.wait()
    for out, index in ((mine, core), (other, 1 - core)):
        select = jnp.where(column == wanted + step * index, 1.0, 0.0).astype(BF16)
        for part in range(2):
            taken = nt_dot(select, rows[:, part * half : (part + 1) * half])
            out[part * size : (part + 1) * size, :] = taken.astype(BF16)
    weights_copy.wait()
    grads[...] = nn_dot(rows[...], weights[...]).astype(BF16)


def own_forward_kernel(
    reaches, place, queries, keys, values, grads, near, own, far,
    sums, stats, lone_out, lone_query, g_lone,
):
    lone = lone_head(reaches)
    lane = lax.broadcasted_iota(jnp.int32, (TILE, HD), 1)
    for slot in range(SENT):
        head = head_of(jnp.int32(slot), lone)
        query = queries[:, columns(head)]
        tiles = (near, own, far)
        scores = nt_dot(query, keys_of(tiles, slot)) + width_bias(reaches, place, head)
        peak = jnp.max(scores, axis=1, keepdims=True)
        terms = jnp.exp2((scores - peak) * SCALE2)
        total = jnp.sum(terms, axis=1, keepdims=True)
        sums[slot] = nn_dot(terms.astype(BF16), values_of(tiles, slot))
        stats[slot] = jnp.where(lane < HD // 2, peak, total)
    cols = columns(lone)
    scores = nt_dot(queries[:, cols], keys[:, cols])
    peak = jnp.max(scores, axis=1, keepdims=True)
    terms = jnp.exp2((scores - peak) * SCALE2)
    total = jnp.sum(terms, axis=1, keepdims=True)
    out = (nn_dot(terms.astype(BF16), values[:, cols]) / total).astype(BF16)
    lone_out[...] = out
    delta = jnp.sum(grads[:, cols].astype(F32) * out.astype(F32), axis=1, keepdims=True)
    norms = jnp.where(lane < HD // 2, peak * SCALE2 + jnp.log2(total), delta)
    part, grad_key, grad_value = backward(
        queries[:, cols], grads[:, cols], norms, keys[:, cols], values[:, cols], 0.0
    )
    lone_query[...] = (part * SCALE).astype(BF16)
    g_lone[:, :HD] = grad_key.astype(BF16)
    g_lone[:, HD:] = grad_value.astype(BF16)


def forward_kernel(
    reaches, place, queries, grads, near, mid, far, sums, stats, attended, norms
):
    lone = lone_head(reaches)
    lane = lax.broadcasted_iota(jnp.int32, (TILE, HD), 1)
    tiles = (near, mid, far)
    spans = (slice(0, TILE), slice(TILE, 2 * TILE))

    def scores_of(slot):
        head = head_of(jnp.int32(slot), lone)
        query = queries[:, columns(head)]
        bias = width_bias(reaches, place, head)
        return [
            nt_dot(query, jnp.concatenate([tile[slot, span, :HD] for tile in tiles], axis=0))
            + jnp.minimum(bias, row)
            for span, row in zip(spans, sides(reaches, head, 2, place[0], place[2]))
        ]

    following = scores_of(0)
    for slot in range(SENT):
        scores = following
        if slot + 1 < SENT:
            following = scores_of(slot + 1)
        own_peak = stats[slot][:, :1]
        peak = jnp.max(jnp.maximum(scores[0], scores[1]), axis=1, keepdims=True)
        peak = jnp.maximum(peak, own_peak)
        terms = [jnp.exp2((part - peak) * SCALE2) for part in scores]
        shrink = jnp.exp2((own_peak - peak) * SCALE2)
        total = stats[slot][:, HD - 1 :] * shrink
        total = total + jnp.sum(terms[0] + terms[1], axis=1, keepdims=True)
        out = sums[slot] * shrink
        for part, span in zip(terms, spans):
            value = jnp.concatenate([tile[slot, span, HD:] for tile in tiles], axis=0)
            out = out + nn_dot(part.astype(BF16), value)
        out = (out / total).astype(BF16)
        attended[:, slot * HD : (slot + 1) * HD] = out
        grad = grads[:, columns(head_of(jnp.int32(slot), lone))]
        delta = jnp.sum(grad.astype(F32) * out.astype(F32), axis=1, keepdims=True)
        norms[slot] = jnp.where(lane < HD // 2, peak * SCALE2 + jnp.log2(total), delta)


def product_kernel(place, mine, partner, attended, partner_attended, *parts):
    size = mine.shape[0] // (2 * len(parts))
    for index, part in enumerate(parts):
        for half in range(2):
            start = (place[4] ^ index) * size + half * len(parts) * size
            span = pl.ds(pl.multiple_of(start, 16), size)
            total = nn_dot(mine[span, :], attended[...]) + nn_dot(partner[span, :], partner_attended[...])
            part[half] = total.astype(BF16)


def backward(query, grad, norms, key, value, bias):
    probs = jnp.exp2((nt_dot(query, key) + bias) * SCALE2 - norms[:, :1])
    slopes = (probs * (nt_dot(grad, value) - norms[:, HD - 1 :])).astype(BF16)
    grad_key = tn_dot(slopes, query) * SCALE
    grad_value = tn_dot(probs.astype(BF16), grad)
    return nn_dot(slopes, key), grad_key, grad_value


def rows_backward_kernel(
    reaches, place, queries, grads, norms, near, mid, far,
    part_query, g_near, g_mid, g_far,
):
    lone = lone_head(reaches)
    for slot in range(SENT):
        head = head_of(jnp.int32(slot), lone)
        cols = columns(head)
        tiles = (near, mid, far)
        part, grad_key, grad_value = backward(
            queries[:, cols], grads[:, cols], norms[slot], keys_of(tiles, slot),
            values_of(tiles, slot), rows_bias(reaches, place, head),
        )
        part_query[slot] = part
        for index, out in enumerate((g_near, g_mid, g_far)):
            span = slice(2 * index * TILE, 2 * (index + 1) * TILE)
            out[slot, :, :HD] = grad_key[span].astype(BF16)
            out[slot, :, HD:] = grad_value[span].astype(BF16)


def own_backward_kernel(
    reaches, place, queries, grads, norms, near, own, far, part_query, lone_query,
    grad_query, g_near, g_own, g_far,
):
    lone = lone_head(reaches)
    for slot in range(SENT):
        head = head_of(jnp.int32(slot), lone)
        cols = columns(head)
        tiles = (near, own, far)
        part, grad_key, grad_value = backward(
            queries[:, cols], grads[:, cols], norms[slot], keys_of(tiles, slot),
            values_of(tiles, slot), width_bias(reaches, place, head),
        )
        grad_query[:, cols] = ((part_query[slot] + part) * SCALE).astype(BF16)
        for index, out in enumerate((g_near, g_own, g_far)):
            span = slice(index * TILE, (index + 1) * TILE)
            out[slot, :, :HD] = grad_key[span].astype(out.dtype)
            out[slot, :, HD:] = grad_value[span].astype(out.dtype)
    grad_query[:, columns(lone)] = lone_query[...]


def width_sum_kernel(mid, from_near, from_far, to_near, to_far):
    for row, out in enumerate((to_near, to_far)):
        span = slice(row * TILE, (row + 1) * TILE)
        total = mid[:, span].astype(F32) + from_near[:, span].astype(F32)
        out[...] = (total + from_far[:, span].astype(F32)).astype(BF16)


def final_sum_kernel(
    reaches, own, width_near, width_far, height_near, height_far, g_lone, grad_key, grad_value
):
    lone = lone_head(reaches)
    for slot in range(SENT):
        cols = columns(head_of(jnp.int32(slot), lone))
        total = own[slot].astype(F32)
        for part in (width_near, width_far, height_near, height_far):
            total = total + part[slot].astype(F32)
        grad_key[:, cols] = total[:, :HD].astype(BF16)
        grad_value[:, cols] = total[:, HD:].astype(BF16)
    cols = columns(lone)
    grad_key[:, cols] = g_lone[:, :HD]
    grad_value[:, cols] = g_lone[:, HD:]


def x_sum_kernel(place, *refs):
    half = (len(refs) - 4) // 2
    parts = refs[2 * half :]
    size = refs[0].shape[1] // len(parts)
    for index, part in enumerate(parts):
        span = pl.ds(pl.multiple_of((place[0] ^ index) * size, 8), size)
        for side in range(2):
            for group, cols in (
                (refs[:half], slice(0, SENT * HD)),
                (refs[half : 2 * half], slice(SENT * HD, HEADS * HD)),
            ):
                total = group[0][side, span, :].astype(F32)
                for ref in group[1:]:
                    total = total + ref[side, span, :].astype(F32)
                part[side, :, cols] = total.astype(BF16)


def z_sum_kernel(reaches, parts, out):
    lone = lone_head(reaches)
    total = parts[0].astype(F32)
    for index in range(1, parts.shape[0]):
        total = total + parts[index].astype(F32)
    for slot in range(SENT):
        out[:, columns(head_of(jnp.int32(slot), lone))] = total[:, slot * HD : (slot + 1) * HD]
    out[:, columns(lone)] = total[:, SENT * HD :]


def y_sum_kernel(first, second, third, fourth, parts):
    count = parts.shape[0] // 2
    size = first.shape[1] // count
    for half in range(2):
        total = first[half].astype(F32) + second[half].astype(F32)
        total = (total + third[half].astype(F32) + fourth[half].astype(F32)).astype(BF16)
        for index in range(count):
            parts[half * count + index] = total[index * size : (index + 1) * size]


def call(kernel, outs, scalars, on_chip=None, flops=10**9, loose=0):
    def run(*args):
        args = [
            a if i < scalars + loose else pltpu.with_memory_space_constraint(a, pltpu.VMEM)
            for i, a in enumerate(args)
        ]
        return pl.pallas_call(
            kernel,
            out_shape=[
                (pltpu.VMEM if inside else pltpu.HBM)(shape, dtype)
                for (shape, dtype), inside in zip(outs, on_chip or [True] * len(outs))
            ],
            in_specs=[SMEM] * scalars + [VMEM] * (len(args) - scalars),
            out_specs=[VMEM] * len(outs),
            compiler_params=pltpu.CompilerParams(vmem_limit_bytes=20 << 20),
            cost_estimate=pl.CostEstimate(
                flops=flops, transcendentals=0, bytes_accessed=1 << 20
            ),
        )(*args)

    return run


def in_hbm(array):
    return pltpu.with_memory_space_constraint(array, pltpu.HBM)


def with_near(block, axis):
    return lax.ppermute(block, axis, [(i, i ^ 1) for i in range(lax.axis_size(axis))])


def with_far(block, axis):
    count = lax.axis_size(axis)
    return lax.ppermute(block, axis, [(i, ((i + 1) ^ 1) - 1) for i in range(1, count - 1)])


def with_others(parts, axis):
    count = len(parts)
    pairs = [[(i, i ^ m) for i in range(count)] for m in range(count)]
    sent = {m: lax.ppermute(parts[m], axis, pairs[m]) for m in (2, 1, 3)}
    return [parts[0]] + [sent[m] for m in range(1, count)]


def grads_of(queries, key_tiles, value_tiles, out_grad, w_out, reaches):
    shape = queries.shape
    width = shape[5]
    model_width = out_grad.shape[5]
    zh, x, ha, zl = (lax.axis_size(axis) for axis in ("zh", "x", "ha", "zl"))
    place = jnp.stack(
        [
            lax.axis_index("ha"), lax.axis_index(WIDTH), jnp.int32(ha), jnp.int32(2 * zl),
            lax.axis_index("x"),
        ]
    ).astype(jnp.int32)
    queries = queries.reshape(TILE, width)
    keys = key_tiles.reshape(TILE, width)
    values = value_tiles.reshape(TILE, width)
    grad_rows = out_grad.reshape(TILE, model_width)

    tile = ((SENT, TILE, 2 * HD), BF16)
    pair = ((SENT, 2 * TILE, 2 * HD), BF16)
    flat = ((TILE, width), BF16)
    head = ((SENT, TILE, HD), F32)
    own = pl.pallas_call(
        pack_kernel,
        out_shape=pltpu.VMEM(*tile),
        in_specs=[SMEM, HBM, HBM],
        out_specs=VMEM,
        scratch_shapes=[pltpu.SemaphoreType.DMA((SENT, 2))],
        compiler_params=pltpu.CompilerParams(vmem_limit_bytes=20 << 20),
    )(in_hbm(reaches), in_hbm(keys), in_hbm(values))
    row_near = with_near(own, "ha")
    row_far = with_far(own, "ha")
    far = with_far(own, WIDTH)
    near = with_near(own, WIDTH)
    half = ((model_width // 2, TILE), BF16)
    step = model_width // (zh * x * ha * zl * 2)
    assert all(j * ((1 << 18) // step + 1) >> 18 == j // step for j in range(model_width // 4))
    grads, mine, other = pl.pallas_call(
        functools.partial(rows_kernel, step),
        out_shape=[pltpu.VMEM(*shape) for shape in (flat, half, half)],
        in_specs=[SMEM, HBM, HBM],
        out_specs=[VMEM] * 3,
        scratch_shapes=[
            pltpu.VMEM(grad_rows.shape, BF16), pltpu.VMEM(w_out.shape, BF16),
            pltpu.SemaphoreType.DMA((2,)),
        ],
        compiler_params=pltpu.CompilerParams(vmem_limit_bytes=20 << 20),
        cost_estimate=pl.CostEstimate(
            flops=10**9, transcendentals=0, bytes_accessed=1 << 20
        ),
    )(place, in_hbm(grad_rows), in_hbm(w_out))
    row_near, row_far, grads = lax.optimization_barrier((row_near, row_far, grads))
    (mid_rows,) = call(stack_kernel, [pair], 0)(row_near, row_far)
    far_rows = with_far(mid_rows, WIDTH)
    near_rows = with_near(mid_rows, WIDTH)
    partner = with_near(other, "core")
    small = ((TILE, HD), BF16)
    sums, stats, lone_out, lone_query, g_lone = call(
        own_forward_kernel, [head, head, small, small, ((TILE, 2 * HD), BF16)], 2
    )(reaches, place, queries, keys, values, grads, near, own, far)
    size = model_width // (4 * x)
    lone_parts = call(product_kernel, [((2, size, HD), BF16)] * x, 1)(
        place, mine, partner, lone_out, with_near(lone_out, "core")
    )
    lone_parts = with_others(lone_parts, "x")
    attended, norms = call(forward_kernel, [((TILE, SENT * HD), BF16), head], 2)(
        reaches, place, queries, grads, near_rows, mid_rows, far_rows, sums, stats
    )

    parts = call(product_kernel, [((2, size, SENT * HD), BF16)] * x, 1)(
        place, mine, partner, attended, with_near(attended, "core")
    )
    parts, norms = lax.optimization_barrier((parts, norms))
    parts = with_others(parts, "x")
    parts = call(x_sum_kernel, [((2, size // ha, width), BF16)] * ha, 1)(
        place, *parts, *lone_parts
    )
    parts = with_others(parts, "ha")
    (summed,) = call(y_sum_kernel, [((zh * zl, size // (ha * zl), width), BF16)], 0)(*parts)

    part_query, g_near, g_mid, g_far = call(rows_backward_kernel, [head, pair, pair, pair], 2)(
        reaches, place, queries, grads, norms, near_rows, mid_rows, far_rows
    )
    from_far = with_far(g_far, WIDTH)
    from_near = with_near(g_near, WIDTH)
    grad_query, g_near, g_own, g_far = call(
        own_backward_kernel, [flat, tile, tile, tile], 2, [False, True, False, True]
    )(reaches, place, queries, grads, norms, near, own, far, part_query, lone_query)
    width_far = with_far(g_far, WIDTH)
    width_near = with_near(g_near, WIDTH)
    to_near, to_far = call(width_sum_kernel, [tile, tile], 0)(g_mid, from_near, from_far)
    summed, _ = lax.optimization_barrier((summed, to_near))
    height_near = with_near(to_near, "ha")
    height_far = with_far(to_far, "ha")
    parts = lax.all_to_all(summed, ("zh", "zl"), 0, 0, tiled=True)
    (grad_w_out,) = call(z_sum_kernel, [(parts.shape[1:], F32)], 1, [False])(reaches, parts)
    grad_key, grad_value = call(final_sum_kernel, [flat, flat], 1, [False, False], loose=1)(
        reaches, in_hbm(g_own), width_near, width_far, height_near, height_far, g_lone
    )
    return (
        grad_query.reshape(shape), grad_key.reshape(shape), grad_value.reshape(shape), grad_w_out,
    )


def solution(mesh):
    dp, ha, wa = mesh.devices.shape
    split = Mesh(mesh.devices.reshape(2, dp // 2, ha, wa // 2, 2), ("zh", "x", "ha", "zl", "core"))
    tiles = P(("zh", "x"), None, "ha", WIDTH, None, None)
    return jax.shard_map(
        grads_of,
        mesh=split,
        in_specs=(tiles, tiles, tiles, tiles, P(), P()),
        out_specs=(tiles, tiles, tiles, P(("zh", "x", "ha", "zl", "core"), None)),
        check_vma=False,
    )
```
